32 devices in a mesh: sx: 8 (over y, x, core), sy: 4 (over z).
Axes of the slice: x: 2, y: 2, z: 4, core: 2. Of those that a mesh axis runs over, the one named last changes fastest.
Arguments:
- queries: bfloat16 [2048, 32, 128], P(('sx', 'sy')), may hold values from -8 to 8
- keys: bfloat16 [2048, 4, 128], P(('sx', 'sy')), may hold values from -8 to 8
- values: bfloat16 [2048, 4, 128], P(('sx', 'sy')), may hold values from -6 to 6
Outputs:
- attention: bfloat16 [2048, 32, 128], P(('sx', 'sy'))
The draws below stay inside these ranges and needn't reach their ends.
All inputs are finite; a program needn't handle non-finite values.
Results may differ from the reference program's by a relative error of at most 0.005.
Values may be sent and summed in bfloat16 or wider, within the bound.
A program may use at most 64 MiB of HBM per device.

```python
import math
import jax
import jax.numpy as jnp
from jax import lax

HEAD_DIM = 128
HEADS = 32
KV_HEADS = 4
TOKENS = 2048


def shard_levels(own_key, dims, shards, low, high):
    loudness = 1.0
    for axis_at, shards_of in shards:
        heights = jax.random.uniform(jax.random.fold_in(jax.random.fold_in(own_key, 6), axis_at), (shards_of,), jnp.float32, low / len(shards), high / len(shards))
        loudness = loudness * jnp.repeat(jnp.exp(heights), dims[axis_at] // shards_of).reshape((-1,) + (1,) * (len(dims) - 1 - axis_at))
    return loudness


def noise(key, shape, width, most, cuts=(), kind=jnp.bfloat16):
    entries = jax.random.normal(key, shape, jnp.float32) * width
    if len(cuts) > 0:
        entries = shard_levels(key, shape, cuts, -0.22, 0.18) * entries
    return jnp.clip(entries, min=-most, max=most).astype(kind)


def setup_inputs(seed: int = 0) -> dict:
    key_of = jax.random.split(jax.random.key(seed), 4)
    return {
        "queries": noise(key_of[0], (TOKENS, HEADS, HEAD_DIM), 1.6, 8.0, ((0, 32),)),
        "keys": noise(key_of[1], (TOKENS, KV_HEADS, HEAD_DIM), 1.6, 8.0, ((0, 32),)),
        "values": noise(key_of[2], (TOKENS, KV_HEADS, HEAD_DIM), 1.0, 6.0, ((0, 32),)),
    }


def frequencies(head_width):
    half_index = jnp.arange(head_width // 2, dtype=jnp.float32)
    base_rate = jnp.power(jnp.float32(500000.0), -2.0 * half_index / head_width)
    wavelen = 2.0 * math.pi / base_rate
    smooth = (8192.0 / wavelen - 1.0) / 3.0
    blended = (1.0 - smooth) * base_rate / 8.0 + smooth * base_rate
    return jnp.where(wavelen < 2048.0, base_rate, jnp.where(wavelen > 8192.0, base_rate / 8.0, blended))

def rotate(heads_in, positions):
    head_width = heads_in.shape[-1]
    half_width = head_width // 2
    angles = positions.astype(jnp.float32)[:, None] * frequencies(head_width)[None, :]
    cosine = jnp.cos(angles)[:, None, :]
    sine_wave = jnp.sin(angles)[:, None, :]
    widened = heads_in.astype(jnp.float32)
    front = widened[..., :half_width]
    second = widened[..., half_width:]
    turned = jnp.concatenate([front * cosine - second * sine_wave, second * cosine + front * sine_wave], axis=-1)
    return turned.astype(jnp.bfloat16)

def reference(queries, keys, values):
    total_rows, heads_all, head_width = queries.shape
    group_size = heads_all // keys.shape[1]
    positions = jnp.arange(total_rows, dtype=jnp.int32)
    query_rot = lax.optimization_barrier(rotate(queries, positions))
    key_rot = lax.optimization_barrier(rotate(keys, positions))
    score_scale = 1.0 / math.sqrt(head_width)
    block_size = total_rows // 8

    def one_head(head_index):
        query_head = lax.dynamic_index_in_dim(query_rot, head_index, 1, keepdims=False)
        key_index = (head_index // group_size).astype(jnp.int32)
        key_head = lax.dynamic_index_in_dim(key_rot, key_index, 1, keepdims=False)
        value_head = lax.dynamic_index_in_dim(values, key_index, 1, keepdims=False)
        pieces = []
        for block_index in range(8):
            row_begin = block_index * block_size
            key_end = row_begin + block_size
            query_rows = query_head[row_begin:key_end]
            scores = jnp.dot(query_rows, key_head[:key_end].T, preferred_element_type=jnp.float32) * score_scale
            allowed = positions[:key_end][None, :] <= positions[row_begin:key_end][:, None]
            scores = jnp.where(allowed, scores, -jnp.inf)
            weights = jnp.exp(scores - lax.optimization_barrier(jnp.max(scores, axis=1, keepdims=True)))
            summed = jnp.dot(weights.astype(jnp.bfloat16), value_head[:key_end], preferred_element_type=jnp.float32)
            pieces.append(summed / lax.optimization_barrier(jnp.sum(weights, axis=1, keepdims=True)))
        return jnp.concatenate(pieces, axis=0).astype(jnp.bfloat16)
    result = lax.map(one_head, jnp.arange(heads_all, dtype=jnp.int32))
    return jnp.transpose(result, (1, 0, 2))
```

```python
import functools
import math

import jax
import jax.numpy as jnp
from jax import lax
from jax.experimental import pallas as pl
from jax.experimental.pallas import tpu as pltpu
from jax.sharding import PartitionSpec as P

MESH = pl.DeviceIdType.MESH


def frequencies(head_width):
    half_index = jnp.arange(head_width // 2, dtype=jnp.float32)
    base_rate = jnp.power(jnp.float32(500000.0), -2.0 * half_index / head_width)
    wavelen = 2.0 * math.pi / base_rate
    smooth = (8192.0 / wavelen - 1.0) / 3.0
    blended = (1.0 - smooth) * base_rate / 8.0 + smooth * base_rate
    return jnp.where(
        wavelen < 2048.0, base_rate, jnp.where(wavelen > 8192.0, base_rate / 8.0, blended)
    )


def rotate(heads_in, cosine, sine_wave):
    half_width = heads_in.shape[-1] // 2
    widened = heads_in.astype(jnp.float32)
    front = widened[..., :half_width]
    second = widened[..., half_width:]
    turned = jnp.concatenate(
        [front * cosine - second * sine_wave, second * cosine + front * sine_wave], axis=-1
    )
    return turned.astype(jnp.bfloat16)


def kernel(
    n, m, q_ref, kv_ref, o_ref, qbuf, gath, obuf, top, mass, acc,
    kv_send, kv_recv, q_send, q_recv, up_send, down_send, z_recv, d_send, d_recv, o_send, o_recv,
):
    s = lax.axis_index("sx")
    z = lax.axis_index("sy")
    kv_heads, tok, width = kv_ref.shape[1:]
    ratio = n // kv_heads
    per = q_ref.shape[0] // n
    rows = per * tok
    c = s % ratio
    partner = s - c + (1 - c)
    exponent_scale = math.log2(math.e) / math.sqrt(width)

    barrier = pltpu.get_barrier_semaphore()
    for i in range(1, n):
        pl.semaphore_signal(barrier, inc=1, device_id=((s + i) % n, z), device_id_type=MESH)

    @pl.when(z > 0)
    def _():
        pl.semaphore_signal(barrier, inc=1, device_id=(s, z - 1), device_id_type=MESH)

    @pl.when(z < m - 1)
    def _():
        pl.semaphore_signal(barrier, inc=1, device_id=(s, z + 1), device_id_type=MESH)

    pl.semaphore_wait(barrier, n - 1 + (z > 0).astype(jnp.int32) + (z < m - 1).astype(jnp.int32))

    def remote(src, dst, send, recv, device):
        return pltpu.make_async_remote_copy(
            src_ref=src, dst_ref=dst, send_sem=send, recv_sem=recv, device_id=device, device_id_type=MESH
        )

    def kv_copy(t):
        return remote(
            kv_ref.at[t % ratio, t // ratio], gath.at[t % ratio, z, s], kv_send.at[t], kv_recv.at[s], (t, z)
        )

    def q_copy(t):
        return remote(q_ref.at[pl.ds(t * per, per)], qbuf.at[s], q_send.at[t], q_recv.at[s], (t, z))

    def o_copy(t):
        return remote(obuf.at[t], o_ref.at[pl.ds(s * per, per)], o_send.at[t], o_recv.at[s], (t, z))

    def up_copy(p):
        return remote(gath.at[c, p], gath.at[c, p], up_send.at[p], z_recv.at[p], (s, z + 1))

    def down_copy(p):
        return remote(gath.at[c, p], gath.at[c, p], down_send.at[p], z_recv.at[p], (s, z - 1))

    def across(p):
        return remote(gath.at[c, p], gath.at[c, p], d_send.at[p], d_recv.at[p], (partner, z))

    kv_own = pltpu.make_async_copy(kv_ref.at[c, s // ratio], gath.at[c, z, s], kv_recv.at[s])
    q_own = pltpu.make_async_copy(q_ref.at[pl.ds(s * per, per)], qbuf.at[s], q_recv.at[s])
    kv_own.start()
    for i in range(1, n):
        kv_copy((s + i) % n).start()
    q_own.start()
    for i in range(1, n):
        q_copy((s + i) % n).start()

    for t in range(n):
        top[t] = jnp.full((1, rows), -jnp.inf, jnp.float32)
        mass[t] = jnp.zeros((1, rows), jnp.float32)
        acc[t] = jnp.zeros((width, rows), jnp.float32)

    for i in range(1, n):
        t = (s + i) % n
        pltpu.make_async_copy(gath.at[c, z, t], gath.at[c, z, t], kv_recv.at[t]).wait()
    kv_own.wait()

    @pl.when(z < m - 1)
    def _():
        up_copy(z).start()

    @pl.when(z > 0)
    def _():
        down_copy(z).start()

    across(z).start()

    def landed(p, sem):
        pltpu.make_async_copy(gath.at[c, p], gath.at[c, p], sem.at[p]).wait()

    def relay(d):
        low = z - d
        high = z + d

        @pl.when(low >= 0)
        def _():
            landed(low, z_recv)

            @pl.when(z < m - 1)
            def _():
                up_copy(low).start()

            across(low).start()

        @pl.when(high < m)
        def _():
            landed(high, z_recv)

            @pl.when(z > 0)
            def _():
                down_copy(high).start()

            across(high).start()

    relay(1)
    for i in range(1, n):
        t = (s + i) % n
        pltpu.make_async_copy(qbuf.at[t], qbuf.at[t], q_recv.at[t]).wait()
    q_own.wait()

    def absorb(p):
        pltpu.make_async_copy(gath.at[1 - c, p], gath.at[1 - c, p], d_recv.at[p]).wait()
        keys = gath[0, p].reshape(n * tok, width)
        values_t = gath[1, p].reshape(n * tok, width).T
        for t in range(n):
            blocks = min(n, 2 * (t // 2 + 1))
            count = blocks * tok
            tail = 2 * tok
            query = qbuf[t].reshape(rows, width)
            scores = lax.dot_general(
                keys[:count], query, (((1,), (1,)), ((), ())), preferred_element_type=jnp.float32
            )
            place = lax.broadcasted_iota(jnp.int32, (tail, rows), 0)
            key_place = place % tok + ((blocks - 2 + place // tok) * m + p) * tok
            lane = lax.broadcasted_iota(jnp.int32, (tail, rows), 1)
            query_place = lane % tok + (t * m + z) * tok
            masked = jnp.where(key_place <= query_place, scores[count - tail :], -jnp.inf)
            if count > tail:
                scores = jnp.concatenate([scores[: count - tail], masked], axis=0)
            else:
                scores = masked
            old = top[t]
            new = jnp.maximum(old, jnp.max(scores, axis=0, keepdims=True) * exponent_scale)
            shrink = jnp.exp2(old - new)
            weights = jnp.exp2(scores * exponent_scale - new)
            top[t] = new
            mass[t] = mass[t] * shrink + jnp.sum(weights, axis=0, keepdims=True)
            acc[t] = acc[t] * shrink + jnp.dot(
                values_t[:, :count], weights.astype(jnp.bfloat16), preferred_element_type=jnp.float32
            )

    def step(u, carry):
        @pl.when(u >= 2)
        def _():
            relay(u)

        def side(sign, inner):
            p = z + (2 * sign - 1) * u

            @pl.when((p >= 0) & (p < m) & (u + 1 - sign > 0))
            def _():
                absorb(p)

            return inner

        return lax.fori_loop(0, 2, side, carry)

    lax.fori_loop(0, m, step, 0)

    def finish(t):
        scaled = acc[t] / mass[t]
        return scaled.T.astype(jnp.bfloat16).reshape(per, tok, width)

    def send_out(i, carry):
        t = (s + i) % n
        obuf[t] = finish(t)
        o_copy(t).start()
        return carry

    lax.fori_loop(1, n, send_out, 0)
    o_ref[pl.ds(s * per, per)] = finish(s)

    for i in range(1, n):
        t = (s + i) % n
        kv_copy(t).wait_send()
        q_copy(t).wait_send()
        o_copy(t).wait_send()

    def drain(p, carry):
        @pl.when((z < m - 1) & (p <= z))
        def _():
            up_copy(p).wait_send()

        @pl.when((z > 0) & (p >= z))
        def _():
            down_copy(p).wait_send()

        across(p).wait_send()
        return carry

    lax.fori_loop(0, m, drain, 0)
    for i in range(1, n):
        t = (s + i) % n
        piece = o_ref.at[pl.ds(t * per, per)]
        pltpu.make_async_copy(piece, piece, o_recv.at[t]).wait()


def shards(n, m, queries, keys, values):
    tok, heads, width = queries.shape
    kv_heads = keys.shape[1]
    assert n == 2 * kv_heads and heads % n == 0
    per = heads // n
    rows = per * tok
    start_row = lax.axis_index(("sx", "sy")) * tok
    positions = start_row + jnp.arange(tok, dtype=jnp.int32)
    angles = positions.astype(jnp.float32)[:, None] * frequencies(width)[None, :]
    cosine = jnp.cos(angles)[:, None, :]
    sine_wave = jnp.sin(angles)[:, None, :]
    query_rot = rotate(queries, cosine, sine_wave).transpose(1, 0, 2)
    key_rot = rotate(keys, cosine, sine_wave)
    both = jnp.stack([key_rot, values]).transpose(0, 2, 1, 3)
    vmem = pl.BlockSpec(memory_space=pltpu.VMEM)
    dma = pltpu.SemaphoreType.DMA
    out = pl.pallas_call(
        functools.partial(kernel, n, m),
        out_shape=jax.ShapeDtypeStruct((heads, tok, width), jnp.bfloat16),
        in_specs=[vmem, vmem],
        out_specs=vmem,
        scratch_shapes=[
            pltpu.VMEM((n, per, tok, width), jnp.bfloat16),
            pltpu.VMEM((2, m, n, tok, width), jnp.bfloat16),
            pltpu.VMEM((n, per, tok, width), jnp.bfloat16),
            pltpu.VMEM((n, 1, rows), jnp.float32),
            pltpu.VMEM((n, 1, rows), jnp.float32),
            pltpu.VMEM((n, width, rows), jnp.float32),
            dma((n,)), dma((n,)), dma((n,)), dma((n,)),
            dma((m,)), dma((m,)), dma((m,)), dma((m,)), dma((m,)),
            dma((n,)), dma((n,)),
        ],
        compiler_params=pltpu.CompilerParams(collective_id=0, has_side_effects=True),
    )(query_rot, both)
    return out.transpose(1, 0, 2)


def solution(mesh):
    n, m = mesh.shape["sx"], mesh.shape["sy"]
    placed = P(("sx", "sy"), None, None)
    return jax.shard_map(
        functools.partial(shards, n, m), mesh=mesh, in_specs=(placed,) * 3, out_specs=placed, check_vma=False
    )
```

```python
import functools
import math

import jax
import jax.numpy as jnp
from jax import lax
from jax.experimental import pallas as pl
from jax.experimental.pallas import tpu as pltpu
from jax.sharding import PartitionSpec as P

MESH = pl.DeviceIdType.MESH


def frequencies(head_width):
    half_index = jnp.arange(head_width // 2, dtype=jnp.float32)
    base_rate = jnp.power(jnp.float32(500000.0), -2.0 * half_index / head_width)
    wavelen = 2.0 * math.pi / base_rate
    smooth = (8192.0 / wavelen - 1.0) / 3.0
    blended = (1.0 - smooth) * base_rate / 8.0 + smooth * base_rate
    return jnp.where(
        wavelen < 2048.0, base_rate, jnp.where(wavelen > 8192.0, base_rate / 8.0, blended)
    )


def kernel(
    n, m, queries_ref, keys_ref, values_ref, cos_ref, sin_ref, o_ref, wide, q_ref, kv_ref, qbuf, gath, obuf, top, mass, acc,
    kv_send, kv_recv, q_send, q_recv, up_send, down_send, z_recv, d_send, d_recv, o_send, o_recv,
):
    s = lax.axis_index("sx")
    z = lax.axis_index("sy")
    kv_heads, tok, width = kv_ref.shape[1:]
    ratio = n // kv_heads
    per = q_ref.shape[0] // n
    rows = per * tok
    c = s % ratio
    partner = s - c + (1 - c)
    exponent_scale = math.log2(math.e) / math.sqrt(width)

    pieces = n // ratio

    barrier = pltpu.get_barrier_semaphore()
    for i in range(1, n):
        pl.semaphore_signal(barrier, inc=1, device_id=((s + i) % n, z), device_id_type=MESH)

    @pl.when(z > 0)
    def _():
        pl.semaphore_signal(barrier, inc=1, device_id=(s, z - 1), device_id_type=MESH)

    @pl.when(z < m - 1)
    def _():
        pl.semaphore_signal(barrier, inc=1, device_id=(s, z + 1), device_id_type=MESH)

    cosine = cos_ref[...]
    sine_wave = sin_ref[...]

    def turned(x):
        return (x * cosine + pltpu.roll(x, width // 2, 1) * sine_wave).astype(jnp.bfloat16)

    wide[:, :kv_heads] = keys_ref[...].astype(jnp.float32)
    wide[:, kv_heads : 2 * kv_heads] = values_ref[...].astype(jnp.float32)
    for g in range(kv_heads):
        kv_ref[0, g] = turned(wide[:, g, :])
        kv_ref[1, g] = wide[:, kv_heads + g, :].astype(jnp.bfloat16)

    pl.semaphore_wait(barrier, n - 1 + (z > 0).astype(jnp.int32) + (z < m - 1).astype(jnp.int32))

    def remote(src, dst, send, recv, device):
        return pltpu.make_async_remote_copy(
            src_ref=src, dst_ref=dst, send_sem=send, recv_sem=recv, device_id=device, device_id_type=MESH
        )

    def kv_copy(t):
        return remote(
            kv_ref.at[t % ratio, t // ratio], gath.at[t % ratio, z, s], kv_send.at[t], kv_recv.at[s], (t, z)
        )

    def q_copy(t):
        return remote(q_ref.at[pl.ds(t * per, per)], qbuf.at[s], q_send.at[t], q_recv.at[s], (t, z))

    def o_copy(t):
        return remote(obuf.at[t], o_ref.at[pl.ds(s * per, per)], o_send.at[t], o_recv.at[s], (t, z))

    def part(p, h):
        return gath.at[c, p, pl.ds(h * ratio, ratio)]

    def up_copy(p, h):
        return remote(part(p, h), part(p, h), up_send.at[p, h], z_recv.at[p, h], (s, z + 1))

    def down_copy(p, h):
        return remote(part(p, h), part(p, h), down_send.at[p, h], z_recv.at[p, h], (s, z - 1))

    def across(p, h):
        return remote(part(p, h), part(p, h), d_send.at[p, h], d_recv.at[p, h], (partner, z))

    kv_own = pltpu.make_async_copy(kv_ref.at[c, s // ratio], gath.at[c, z, s], kv_recv.at[s])
    q_own = pltpu.make_async_copy(q_ref.at[pl.ds(s * per, per)], qbuf.at[s], q_recv.at[s])
    kv_own.start()
    for i in range(1, n):
        kv_copy((s + i) % n).start()
    wide[...] = queries_ref[...].astype(jnp.float32)
    for h in range(n * per):
        q_ref[h] = turned(wide[:, h, :])
    for i in range(1, n):
        q_copy((s + i) % n).start()
    q_own.start()

    for t in range(n):
        top[t] = jnp.full((1, rows), -jnp.inf, jnp.float32)
        mass[t] = jnp.zeros((1, rows), jnp.float32)
        acc[t] = jnp.zeros((width, rows), jnp.float32)

    kv_own.wait()
    home = s // ratio

    def first(i, carry):
        h = (home + i) % pieces
        for j in range(ratio):
            t = h * ratio + j

            @pl.when(t != s)
            def _():
                pltpu.make_async_copy(gath.at[c, z, t], gath.at[c, z, t], kv_recv.at[t]).wait()

        @pl.when(z < m - 1)
        def _():
            up_copy(z, h).start()

        @pl.when(z > 0)
        def _():
            down_copy(z, h).start()

        across(z, h).start()
        return carry

    lax.fori_loop(0, pieces, first, 0)

    def relay(d):
        low = z - d
        high = z + d

        def one(i, carry):
            h = (home + i) % pieces

            @pl.when(low >= 0)
            def _():
                pltpu.make_async_copy(part(low, h), part(low, h), z_recv.at[low, h]).wait()

                @pl.when(z < m - 1)
                def _():
                    up_copy(low, h).start()

                across(low, h).start()

            @pl.when(high < m)
            def _():
                pltpu.make_async_copy(part(high, h), part(high, h), z_recv.at[high, h]).wait()

                @pl.when(z > 0)
                def _():
                    down_copy(high, h).start()

                across(high, h).start()

            return carry

        lax.fori_loop(0, pieces, one, 0)

    relay(1)
    relay(2)
    for i in range(1, n):
        t = (s + i) % n
        pltpu.make_async_copy(qbuf.at[t], qbuf.at[t], q_recv.at[t]).wait()
    q_own.wait()

    def absorb(p):
        for h in range(pieces):
            other = gath.at[1 - c, p, pl.ds(h * ratio, ratio)]
            pltpu.make_async_copy(other, other, d_recv.at[p, h]).wait()
        keys = gath[0, p].reshape(n * tok, width)
        values_t = gath[1, p].reshape(n * tok, width).T
        for t in range(n):
            blocks = min(n, 2 * (t // 2 + 1))
            count = blocks * tok
            tail = 2 * tok
            query = qbuf[t].reshape(rows, width)
            scores = lax.dot_general(
                keys[:count], query, (((1,), (1,)), ((), ())), preferred_element_type=jnp.float32
            )
            place = lax.broadcasted_iota(jnp.int32, (tail, rows), 0)
            key_place = place % tok + ((blocks - 2 + place // tok) * m + p) * tok
            lane = lax.broadcasted_iota(jnp.int32, (tail, rows), 1)
            query_place = lane % tok + (t * m + z) * tok
            masked = jnp.where(key_place <= query_place, scores[count - tail :], -jnp.inf)
            if count > tail:
                scores = jnp.concatenate([scores[: count - tail], masked], axis=0)
            else:
                scores = masked
            old = top[t]
            new = jnp.maximum(old, jnp.max(scores, axis=0, keepdims=True) * exponent_scale)
            shrink = jnp.exp2(old - new)
            weights = jnp.exp2(scores * exponent_scale - new)
            top[t] = new
            mass[t] = mass[t] * shrink + jnp.sum(weights, axis=0, keepdims=True)
            acc[t] = acc[t] * shrink + jnp.dot(
                values_t[:, :count], weights.astype(jnp.bfloat16), preferred_element_type=jnp.float32
            )

    def step(u, carry):
        @pl.when(u >= 2)
        def _():
            relay(u + 1)

        def side(sign, inner):
            p = z + (2 * sign - 1) * u

            @pl.when((p >= 0) & (p < m) & (u + 1 - sign > 0))
            def _():
                absorb(p)

            return inner

        return lax.fori_loop(0, 2, side, carry)

    lax.fori_loop(0, m, step, 0)

    def finish(t):
        scaled = acc[t] / mass[t]
        return scaled.T.astype(jnp.bfloat16).reshape(per, tok, width)

    def send_out(i, carry):
        t = (s + i) % n
        obuf[t] = finish(t)

        @pl.when(i > 1)
        def _():
            o_copy((s + i - 1) % n).start()

        return carry

    lax.fori_loop(1, n, send_out, 0)
    o_ref[pl.ds(s * per, per)] = finish(s)
    o_copy((s + n - 1) % n).start()

    for i in range(1, n):
        t = (s + i) % n
        kv_copy(t).wait_send()
        q_copy(t).wait_send()
        o_copy(t).wait_send()

    def drain(p, carry):
        def one(h, inner):
            @pl.when((z < m - 1) & (p <= z))
            def _():
                up_copy(p, h).wait_send()

            @pl.when((z > 0) & (p >= z))
            def _():
                down_copy(p, h).wait_send()

            across(p, h).wait_send()
            return inner

        return lax.fori_loop(0, pieces, one, carry)

    lax.fori_loop(0, m, drain, 0)
    for i in range(1, n):
        t = (s + i) % n
        piece = o_ref.at[pl.ds(t * per, per)]
        pltpu.make_async_copy(piece, piece, o_recv.at[t]).wait()


def shards(n, m, queries, keys, values):
    tok, heads, width = queries.shape
    kv_heads = keys.shape[1]
    assert n == 2 * kv_heads and heads % n == 0
    per = heads // n
    rows = per * tok
    start_row = lax.axis_index(("sx", "sy")) * tok
    positions = start_row + jnp.arange(tok, dtype=jnp.int32)
    angles = positions.astype(jnp.float32)[:, None] * frequencies(width)[None, :]
    cosine = jnp.cos(angles)
    sine_wave = jnp.sin(angles)
    cosine = jnp.concatenate([cosine, cosine], axis=1)
    sine_wave = jnp.concatenate([-sine_wave, sine_wave], axis=1)
    half_precision = 4 * queries.size + 2 * n * m * tok * width
    limit = (2 * half_precision + 8 * queries.size) * 5 // 4 + 8 * 2**20
    vmem = pl.BlockSpec(memory_space=pltpu.VMEM)
    dma = pltpu.SemaphoreType.DMA
    out = pl.pallas_call(
        functools.partial(kernel, n, m),
        out_shape=jax.ShapeDtypeStruct((heads, tok, width), jnp.bfloat16),
        in_specs=[vmem] * 5,
        out_specs=vmem,
        scratch_shapes=[
            pltpu.VMEM((tok, heads, width), jnp.float32),
            pltpu.VMEM((heads, tok, width), jnp.bfloat16),
            pltpu.VMEM((2, kv_heads, tok, width), jnp.bfloat16),
            pltpu.VMEM((n, per, tok, width), jnp.bfloat16),
            pltpu.VMEM((2, m, n, tok, width), jnp.bfloat16),
            pltpu.VMEM((n, per, tok, width), jnp.bfloat16),
            pltpu.VMEM((n, 1, rows), jnp.float32),
            pltpu.VMEM((n, 1, rows), jnp.float32),
            pltpu.VMEM((n, width, rows), jnp.float32),
            dma((n,)), dma((n,)), dma((n,)), dma((n,)),
            *[dma((m, kv_heads))] * 5,
            dma((n,)), dma((n,)),
        ],
        compiler_params=pltpu.CompilerParams(collective_id=0, has_side_effects=True, vmem_limit_bytes=limit),
    )(queries, keys, values, cosine, sine_wave)
    return out.transpose(1, 0, 2)


def solution(mesh):
    n, m = mesh.shape["sx"], mesh.shape["sy"]
    placed = P(("sx", "sy"), None, None)
    return jax.shard_map(
        functools.partial(shards, n, m), mesh=mesh, in_specs=(placed,) * 3, out_specs=placed, check_vma=False
    )
```
